128 devices in a mesh: data: 1, cp: 128 (over z, y, x, core).
Axes of the slice: x: 4, y: 4, z: 4, core: 2. Of those that a mesh axis runs over, the one named last changes fastest.
Arguments:
- x_new: bfloat16 [4096, 5120], P(('data', 'cp'))
- pos_new: int32 [4096], P(('data', 'cp'))
- k_cache: bfloat16 [32768, 8, 128], P(('data', 'cp'))
- v_cache: bfloat16 [32768, 8, 128], P(('data', 'cp'))
- w_q: bfloat16 [5120, 4096], replicated
- w_k: bfloat16 [5120, 1024], replicated
- w_v: bfloat16 [5120, 1024], replicated
- w_o: bfloat16 [4096, 5120], replicated
Outputs:
- output: bfloat16 [4096, 5120], P(('data', 'cp'))
All inputs are finite; a program needn't handle non-finite values.
Results may differ from the reference program's by a relative error of at most 0.00547.
Values are sent between devices in bfloat16 or wider.
A program may use at most 1 GiB of HBM per device.

```python
import math
import numpy as np
import jax
import jax.numpy as jnp
from jax import lax

CP_SIZE = 128
TOK_DEV = 32
CACHE_DEV = 256
MODEL_DIM = 5120
Q_HEADS = 32
KV_HEADS = 8
HEAD_DIM = 128
ROPE_BASE = 500000
Q_BLOCK = 8

TOKENS = CP_SIZE * TOK_DEV
CACHE_LEN = CP_SIZE * CACHE_DEV
GROUP_SIZE = Q_HEADS // KV_HEADS


def plain_order():
    half_dev = TOK_DEV // 2
    row_idx = np.arange(TOKENS)
    device = row_idx // TOK_DEV
    local_idx = row_idx % TOK_DEV
    piece_idx = np.where(local_idx < half_dev, device, 2 * CP_SIZE - 1 - device)
    return (piece_idx * half_dev + local_idx % half_dev).astype(np.int32)


def rotary(values, positions):
    half_dim = HEAD_DIM // 2
    inv_freq = jnp.power(jnp.float32(ROPE_BASE), -(jnp.arange(half_dim, dtype=jnp.float32) * 2.0 / HEAD_DIM))
    angles = positions.astype(jnp.float32)[:, None] * inv_freq[None, :]
    cos_a = jnp.cos(angles)[:, None, :]
    sin_a = jnp.sin(angles)[:, None, :]
    low_half = values[..., :half_dim]
    high_half = values[..., half_dim:]
    return jnp.concatenate([low_half * cos_a - high_half * sin_a, high_half * cos_a + low_half * sin_a], axis=-1)


def setup_inputs(seed: int = 0, part: int = 0) -> dict:
    part_keys = jax.random.split(jax.random.fold_in(jax.random.key(seed), part), 8)
    weight_keys = jax.random.split(jax.random.key(seed + 1), 4)
    token_order = plain_order()
    walk_x = jnp.cumsum(jax.random.normal(part_keys[0], (TOKENS, MODEL_DIM), jnp.float32), axis=0) / math.sqrt(TOKENS)
    x_plain = walk_x + 0.7 * jax.random.normal(part_keys[1], (TOKENS, MODEL_DIM), jnp.float32)
    start_pos = jax.random.randint(part_keys[2], (), CACHE_LEN, 2 * CACHE_LEN, dtype=jnp.int32)
    positions = start_pos + jnp.asarray(token_order)
    cache_shape = (CACHE_LEN, KV_HEADS, HEAD_DIM)
    walk_k = jnp.cumsum(jax.random.normal(part_keys[3], cache_shape, jnp.float32), axis=0) / math.sqrt(CACHE_LEN)
    walk_v = jnp.cumsum(jax.random.normal(part_keys[4], cache_shape, jnp.float32), axis=0) / math.sqrt(CACHE_LEN)
    k_cache = walk_k + 0.4 * jax.random.normal(part_keys[5], cache_shape, jnp.float32)
    v_cache = 1.2 * walk_v + 0.5 * jax.random.normal(part_keys[6], cache_shape, jnp.float32)
    q_width = Q_HEADS * HEAD_DIM
    kv_width = KV_HEADS * HEAD_DIM
    w_q = jax.random.normal(weight_keys[0], (MODEL_DIM, q_width), jnp.float32) / math.sqrt(MODEL_DIM)
    w_k = 1.5 * jax.random.normal(weight_keys[1], (MODEL_DIM, kv_width), jnp.float32) / math.sqrt(MODEL_DIM)
    w_v = jax.random.normal(weight_keys[2], (MODEL_DIM, kv_width), jnp.float32) / math.sqrt(MODEL_DIM)
    w_o = jax.random.normal(weight_keys[3], (q_width, MODEL_DIM), jnp.float32) / math.sqrt(q_width)
    return {
        "x_new": x_plain[token_order].astype(jnp.bfloat16),
        "pos_new": positions,
        "k_cache": k_cache.astype(jnp.bfloat16),
        "v_cache": v_cache.astype(jnp.bfloat16),
        "w_q": w_q.astype(jnp.bfloat16),
        "w_k": w_k.astype(jnp.bfloat16),
        "w_v": w_v.astype(jnp.bfloat16),
        "w_o": w_o.astype(jnp.bfloat16),
    }


def reference(x_new, pos_new, k_cache, v_cache, w_q, w_k, w_v, w_o):
    q_proj = jnp.dot(x_new, w_q, preferred_element_type=jnp.float32).astype(jnp.bfloat16)
    k_proj = jnp.dot(x_new, w_k, preferred_element_type=jnp.float32).astype(jnp.bfloat16)
    v_new = jnp.dot(x_new, w_v, preferred_element_type=jnp.float32).astype(jnp.bfloat16).reshape(TOKENS, KV_HEADS, HEAD_DIM)
    q_rot = rotary(q_proj.astype(jnp.float32).reshape(TOKENS, Q_HEADS, HEAD_DIM), pos_new).astype(jnp.bfloat16)
    k_new = rotary(k_proj.astype(jnp.float32).reshape(TOKENS, KV_HEADS, HEAD_DIM), pos_new).astype(jnp.bfloat16)
    keys_all = jnp.concatenate([k_cache, k_new], axis=0).astype(jnp.float32)
    vals_all = jnp.concatenate([v_cache, v_new], axis=0).astype(jnp.float32)
    key_pos = jnp.concatenate([jnp.full((CACHE_LEN,), -1, jnp.int32), pos_new])
    score_scale = 1.0 / math.sqrt(HEAD_DIM)
    q_blocks = q_rot.reshape(TOKENS // Q_BLOCK, Q_BLOCK, KV_HEADS, GROUP_SIZE, HEAD_DIM)
    pos_blocks = pos_new.reshape(TOKENS // Q_BLOCK, Q_BLOCK)

    def attend(block_args):
        q_blk, q_pos = block_args
        scores = jnp.einsum("qkgd,ckd->qkgc", q_blk.astype(jnp.float32), keys_all) * score_scale
        visible = key_pos[None, :] <= q_pos[:, None]
        scores = jnp.where(visible[:, None, None, :], scores, -jnp.inf)
        row_max = jnp.max(scores, axis=-1, keepdims=True)
        exp_scores = jnp.exp(scores - row_max)
        row_sum = jnp.sum(exp_scores, axis=-1)
        prob_bf16 = exp_scores.astype(jnp.bfloat16).astype(jnp.float32)
        weighted = jnp.einsum("qkgc,ckd->qkgd", prob_bf16, vals_all)
        return (weighted / row_sum[..., None]).astype(jnp.bfloat16)

    attn_out = lax.map(attend, (q_blocks, pos_blocks)).reshape(TOKENS, Q_HEADS * HEAD_DIM)
    proj_out = jnp.dot(attn_out, w_o, preferred_element_type=jnp.float32)
    return (x_new.astype(jnp.float32) + proj_out).astype(jnp.bfloat16)
```

```python
import math

import jax
import jax.numpy as jnp
from jax import lax
from jax.experimental import pallas as pl
from jax.experimental.pallas import tpu as pltpu
from jax.sharding import PartitionSpec as P

ROPE_BASE = 500000.0
F32 = jnp.float32
BF16 = jnp.bfloat16
HD = 128
SUB = 8
HEADS = 8
TOK = 32
HALF = TOK // 2
PAIR = 2 * TOK
CACHE = 256
QB = 512
KT = 2048
KN = 1024
RC = 256
SCALE2 = (1.0 / math.sqrt(HD)) * math.log2(math.e)
MODEL = 5120
GRP = 512
WCOLS = GRP + 2 * HD
QCOLS = 4096
OHALF = MODEL // 2
KSTEP = 2560
OSTEP = 2048
OTILES = (WCOLS, WCOLS, WCOLS, CACHE)
LAST_POS = 4064
PIECES = (0, 4, 1, 3, 5, 7, 2, 6)
TILES = 0xEE7DA5
BLOCKS = 0xFAD244
NEG = float(jnp.finfo(jnp.float32).min)
ACC = slice(HD)
MROW = slice(HD, HD + SUB)
LROW = slice(HD + SUB, HD + 2 * SUB)
STAT = HD + 2 * SUB
KROWS = slice(CACHE)
VLO = slice(CACHE, CACHE + HD)
VHI = slice(CACHE + HD, 2 * CACHE)


def dev(x, y, z, c):
    return ((z * 4 + y) * 4 + x) * 2 + c


def rel_pos(d, t):
    return jnp.where(t < HALF, HALF * d + t, LAST_POS - HALF * d + t)


def rcopy(src, dst, ss, rs, d):
    return pltpu.make_async_remote_copy(
        src_ref=src, dst_ref=dst, send_sem=ss, recv_sem=rs, device_id={"cp": d},
        device_id_type=pl.DeviceIdType.MESH)


def drain(ref, sem):
    pltpu.make_async_copy(ref, ref, sem).wait()


def unless(cond, run, other=None):
    pl.when(jnp.logical_not(cond))(run)
    if other is not None:
        pl.when(cond)(other)


def kernel(
    x_hbm, k_hbm, v_hbm, cos_ref, sin_ref, wq, wk, wv, wo, out_hbm,
    xbuf, kraw, kvsrc, kvt, kvn, newbuf, qbuf, qt, qsend, nsend, accs, cb_core, cb_y, sbuf,
    wbuf, osend, obuf, olhs, kpos, ysend, ybuf,
    loc_sem, w_sem, x_sem, kv1_s, kv1_r, kvx_s, kvx_r, q_s, q_r, qd_s, qd_r,
    n_s, n_r, nx_s, nx_r, cc_s, cc_r, cy_s, cy_r, o_s, o_r, od_s, od_r, y_s, y_r,
):
    me = lax.axis_index("cp")
    c = lax.rem(me, 2)
    x = lax.rem(me // 2, 4)
    y = lax.rem(me // 8, 4)
    z = me // 32
    nc = 1 - c
    half_b = y // 2
    s = lax.rem(y, 2)
    head = 2 * z + half_b
    src_core = head // 4
    here = z * 4 + y
    mate = dev(x, y, z, nc)
    xr, xl, xo = (lax.rem(x + i, 4) for i in (1, 3, 2))
    my_tok = pl.ds(pl.multiple_of(c * TOK, TOK), TOK)
    mate_tok = pl.ds(pl.multiple_of(nc * TOK, TOK), TOK)

    def wcopies(i):
        h = 4 * c + i
        cols = pl.ds(pl.multiple_of(h * HD, HD), HD)
        return [
            pltpu.make_async_copy(wq.at[:, pl.ds(pl.multiple_of(h * GRP, GRP), GRP)], wbuf.at[i, :, pl.ds(0, GRP)], w_sem.at[i]),
            pltpu.make_async_copy(wk.at[:, cols], wbuf.at[i, :, pl.ds(GRP, HD)], w_sem.at[i]),
            pltpu.make_async_copy(wv.at[:, cols], wbuf.at[i, :, pl.ds(GRP + HD, HD)], w_sem.at[i]),
        ]

    def wo_copy(n):
        wide = OTILES[n]
        cols = pl.ds(pl.multiple_of(c * OHALF, HD) + n * WCOLS, wide)
        return pltpu.make_async_copy(wo.at[:, cols], wbuf.at[n, pl.ds(0, QCOLS), pl.ds(0, wide)], w_sem.at[4 + n])

    first = [
        pltpu.make_async_copy(k_hbm, kraw.at[0], loc_sem.at[0]),
        pltpu.make_async_copy(v_hbm, kraw.at[1], loc_sem.at[1]),
        pltpu.make_async_copy(x_hbm, xbuf.at[my_tok, :], loc_sem.at[2]),
    ]
    for cp in first:
        cp.start()

    barrier = pltpu.get_barrier_semaphore()

    def greet(d):
        pl.semaphore_signal(barrier, inc=1, device_id={"cp": d}, device_id_type=pl.DeviceIdType.MESH)

    greet(mate)
    for xx in (xr, xl, xo):
        greet(dev(xx, y, z, c))

    def greet_chip(i, _):
        for cc in range(2):
            pl.when(i != here)(lambda: greet(dev(x, lax.rem(i, 4), i // 4, cc)))
        return _

    lax.fori_loop(0, 16, greet_chip, 0)

    for cp in first:
        cp.wait()
    for i in range(4):
        for cp in wcopies(i):
            cp.start()
    for hb in range(2):
        rows = slice(hb * HD, (hb + 1) * HD)
        kh = pltpu.einshape("abc->bac", kraw[0, rows])
        vh = pltpu.einshape("abc->bac", kraw[1, rows])
        for h in range(HEADS):
            kvsrc[h, rows, :] = kh[h]
            kvsrc[h, (VLO, VHI)[hb], :] = vh[h].T
    kvt[0, 0] = kvsrc[head]

    accs[:, ACC, :] = jnp.zeros((HEADS, HD, QB), F32)
    accs[:, MROW, :] = jnp.full((HEADS, SUB, QB), NEG, F32)
    accs[:, LROW, :] = jnp.zeros((HEADS, SUB, QB), F32)
    for xs in range(4):
        row = lax.broadcasted_iota(jnp.int32, (RC, HD), 0)
        r = row // TOK
        zs = lax.rem(z + lax.rem(r, 4), 4)
        ys = jnp.where(r >= 4, 3 - y, y)
        kpos[xs] = rel_pos(dev((x, xl, xr, xo)[xs], ys, zs, c), lax.rem(row, TOK))

    pl.semaphore_wait(barrier, 34)

    x_ex = rcopy(x_hbm, xbuf.at[my_tok, :], x_sem.at[0], x_sem.at[1], mate)
    x_ex.start()

    def slot(xs, p):
        return kvt.at[p // 4 * 2 + xs // 2, xs % 2 * 4 + p % 4]

    def ring_send(p):
        rcopy(slot(0, p), slot(1, p), kvx_s, kvx_r.at[1, p // 4], dev(xr, y, z, c)).start()
        rcopy(slot(0, p), slot(2, p), kvx_s, kvx_r.at[2, p // 4], dev(xl, y, z, c)).start()

    def stage1_send(p):
        r = PIECES[p]
        zd = lax.rem(z + 4 - r % 4, 4)
        yd = 3 - y if r >= 4 else y
        rcopy(kvsrc.at[2 * zd + yd // 2], slot(0, p), kv1_s, kv1_r.at[p], dev(x, yd, zd, c)).start()

    def stage1_arrive(p):
        drain(slot(0, p), kv1_r.at[p])
        ring_send(p)

    def ring_wait(xs, half):
        drain(kvt.at[0, pl.ds(0, 4)], kvx_r.at[xs, half])

    def forward(src, p):
        to = xr if src == 1 else xl
        rcopy(slot(src, p), slot(3, p), kvx_s, kvx_r.at[3, p // 4], dev(to, y, z, c)).start()

    for p in range(1, 4):
        stage1_send(p)
    ring_send(0)

    x_ex.wait_recv()

    def q_dst(i, ss, tau):
        h = 4 * c + i
        return dev(x, 2 * lax.rem(h, 2) + ss, h // 2, tau)

    def q_copy(i, ss, tau):
        return rcopy(qsend.at[i, tau], qbuf.at[tau, here], q_s, q_r.at[here // 4], q_dst(i, ss, tau))

    def n_dst(i):
        h = 4 * c + i
        zd = h // 2
        same = lax.rem(h, 2) == half_b
        return dev(x, jnp.where(same, y, 3 - y), zd, 0), jnp.where(same, 0, 4) + lax.rem(z + 4 - zd, 4)

    def n_copy(i, tau):
        d, r = n_dst(i)
        return rcopy(nsend.at[i, tau], newbuf.at[0, r], n_s, n_r, d + tau)

    cosv = jnp.concatenate([cos_ref[...]] * 2, axis=1)
    sinv = jnp.concatenate([-sin_ref[...], sin_ref[...]], axis=1)

    def rot(u):
        u = u.astype(F32)
        return (u * cosv + pltpu.roll(u, HD // 2, 1) * sinv).astype(BF16)

    for i in range(4):
        drain(wbuf.at[i], w_sem.at[i])
        acc = None
        for k in range(0, MODEL, KSTEP):
            ks = pl.ds(k, KSTEP)
            d = jnp.dot(xbuf[:, ks], wbuf[i, ks, :], preferred_element_type=F32)
            acc = d if acc is None else acc + d
        wo_copy(i).start()
        proj = acc.astype(BF16)
        for g in range(4):
            ro = rot(proj[:, g * HD:(g + 1) * HD])
            for tau in range(2):
                qsend[i, tau, g * TOK:(g + 1) * TOK, :] = ro[tau * TOK:(tau + 1) * TOK]
        kn = rot(proj[:, GRP:GRP + HD])
        vn = proj[:, GRP + HD:]
        for tau in range(2):
            rows = slice(tau * TOK, (tau + 1) * TOK)
            nsend[i, tau, :TOK, :] = kn[rows]
            nsend[i, tau, TOK:, :] = vn[rows]

        def keep_q(tau):
            qbuf[tau, here] = qsend[i, tau]

        def keep_n(tau):
            newbuf[0, 0] = nsend[i, tau]

        for tau in range(2):
            for ss in range(2):
                unless(q_dst(i, ss, tau) == me, lambda: q_copy(i, ss, tau).start(), lambda: keep_q(tau))
            unless(n_dst(i)[0] + tau == me, lambda: n_copy(i, tau).start(), lambda: keep_n(tau))
        for p in ((), (1, 2), (3,), ())[i]:
            stage1_arrive(p)

    def transpose_q(tau, zq):
        for yq in range(4):
            qt[tau * 4 + zq, :, yq * HD:(yq + 1) * HD] = qbuf[tau, zq * 4 + yq].T

    for zq in range(4):
        rows = pl.ds(zq * 4, 4)
        unless(jnp.logical_and(zq == z, c == src_core),
               lambda: drain(qbuf.at[c, rows], q_r.at[zq]),
               lambda: drain(qbuf.at[c, pl.ds(zq * 4, 3)], q_r.at[zq]))
        rcopy(qbuf.at[c, rows], qbuf.at[c, rows], qd_s, qd_r.at[zq], mate).start()
        transpose_q(c, zq)

    unless(c == src_core, lambda: drain(newbuf.at[0], n_r), lambda: drain(newbuf.at[0, pl.ds(1, HEADS - 1)], n_r))
    for k, xx in enumerate((xr, xl, xo)):
        rcopy(newbuf.at[0], newbuf.at[k + 1], nx_s, nx_r, dev(xx, y, z, c)).start()

    for p in range(4, HEADS):
        stage1_send(p)

    for zq in range(4):
        drain(qbuf.at[nc, pl.ds(zq * 4, 4)], qd_r.at[zq])
        transpose_q(nc, zq)

    def fold(op, v):
        return op(v.reshape(RC // SUB, SUB, QB), axis=0)

    def spread(v):
        return v.reshape(-1, SUB, QB)

    def q_pos(qb):
        lane = lax.broadcasted_iota(jnp.int32, (SUB, QB), 1)
        return rel_pos(dev(x, lane // HD, lax.rem(qb, 4), qb // 4), lax.rem(lane, TOK))

    def score_chunk(par, ref, qb, ch, mx, masked):
        sc = jnp.dot(ref[ch, KROWS, :], qt[qb], preferred_element_type=F32)
        if masked:
            kp = spread(jnp.concatenate([kpos[ch]] * (QB // HD), axis=1))
            sc = jnp.where(kp <= q_pos(qb)[None], spread(sc), -jnp.inf).reshape(RC, QB)
        sbuf[par, pl.ds(ch * RC, RC), :] = sc
        f = fold(jnp.max, sc)
        return f if mx is None else jnp.maximum(mx, f)

    def scores(par, ref, qb, masked=False):
        mx = None
        for ch in range(ref.shape[0]):
            mx = score_chunk(par, ref, qb, ch, mx, masked)
        return mx

    def step(par, mx, ref, qb, nref, nqb, masked=False):
        m_old = accs[qb, MROW, :]
        mn = jnp.maximum(m_old, jnp.broadcast_to(jnp.max(mx, axis=0, keepdims=True), (SUB, QB)))
        a = jnp.exp2((m_old - mn) * SCALE2)
        mx2 = ls = pv = None
        for ch in range(ref.shape[0]):
            mx2 = score_chunk(1 - par, nref, nqb, ch, mx2, masked)
            p = jnp.exp2((spread(sbuf[par, pl.ds(ch * RC, RC), :]) - mn[None]) * SCALE2)
            f = jnp.sum(p, axis=0)
            ls = f if ls is None else ls + f
            vt = jnp.concatenate([ref[ch, VLO, :], ref[ch, VHI, :]], axis=1)
            d = jnp.dot(vt, p.reshape(RC, QB).astype(BF16), preferred_element_type=F32)
            pv = d if pv is None else pv + d
        accs[qb, ACC, :] = (spread(accs[qb, ACC, :]) * a[None]).reshape(HD, QB) + pv
        accs[qb, MROW, :] = mn
        accs[qb, LROW, :] = accs[qb, LROW, :] * a + ls
        return mx2

    def tile_pass(ref, masked=False, beside=()):
        def body(it, mx):
            qb = 2 * it
            mx = step(0, mx, ref, qb, ref, qb + 1, masked)
            mx = step(1, mx, ref, qb + 1, ref, lax.rem(qb + 2, HEADS), masked)
            for k, run in enumerate(beside):
                pl.when(it == k)(run)
            return mx

        lax.fori_loop(0, HEADS // 2, body, scores(0, ref, 0, masked))

    def ring_pass(src, half):
        ring_wait(src, half)
        for p in range(2):
            forward(src, 4 * half + 2 * src - 2 + p)

    ring_pass(1, 0)

    def arrive(*ps):
        def run():
            for p in ps:
                stage1_arrive(p)
        return run

    tile_pass(kvt.at[0], beside=(lambda: ring_pass(2, 0), arrive(4), arrive(5), arrive(6, 7)))

    drain(newbuf.at[pl.ds(1, 3)], nx_r)
    for xs in range(4):
        for r in range(HEADS):
            kvn[xs, r * TOK:(r + 1) * TOK, :] = newbuf[xs, r, :TOK, :]
        for hf in range(2):
            vblk = jnp.concatenate([newbuf[xs, hf * 4 + r, TOK:, :] for r in range(4)], axis=0)
            kvn[xs, (VLO, VHI)[hf], :] = vblk.T

    tile_pass(kvn, True)

    ring_wait(3, 0)

    def blk(u):
        cc = jnp.where(lax.rem(u // 2, 2) == 0, nc, c)
        return 4 * jnp.where(u < 4, 1 - s, s) + 2 * cc + lax.rem(u, 2)

    def cc_copy(k):
        return rcopy(accs.at[blk(k + k // 2 * 2)], cb_core.at[k], cc_s, cc_r.at[k], mate)

    y_mate = dev(x, 2 * half_b + 1 - s, z, c)

    def cy_copy(k):
        return rcopy(accs.at[blk(k + 2)], cb_y.at[k], cy_s, cy_r.at[k], y_mate)

    def merge(dst, src):
        m0, m1 = accs[dst, MROW, :], src[MROW, :]
        mn = jnp.maximum(m0, m1)
        e0, e1 = jnp.exp2((m0 - mn) * SCALE2), jnp.exp2((m1 - mn) * SCALE2)
        accs[dst, ACC, :] = (spread(accs[dst, ACC, :]) * e0[None] + spread(src[ACC, :]) * e1[None]).reshape(HD, QB)
        accs[dst, MROW, :] = mn
        accs[dst, LROW, :] = accs[dst, LROW, :] * e0 + src[LROW, :] * e1

    def tail(it, mx):
        @pl.when(it == 1)
        def _():
            ring_pass(1, 1)
            ring_pass(2, 1)

        pl.when(it == 4)(lambda: ring_wait(3, 1))

        def at(i):
            return jnp.bitwise_and(TILES >> (2 * i), 3), 2 * jnp.bitwise_and(BLOCKS >> (2 * i), 3)

        k0, u0 = at(it)
        k1, u1 = at(jnp.minimum(it + 1, 11))
        mx = step(0, mx, kvt.at[k0], blk(u0), kvt.at[k0], blk(u0 + 1))
        mx = step(1, mx, kvt.at[k0], blk(u0 + 1), kvt.at[k1], blk(u1))

        @pl.when(it == 5)
        def _():
            cc_copy(0).start()
            cc_copy(1).start()

        @pl.when(it == 6)
        def _():
            for k in range(2):
                cc_copy(k).wait_recv()
                merge(blk(2 + k), cb_core.at[k])
                cy_copy(k).start()

        @pl.when(it == 9)
        def _():
            cc_copy(2).start()
            cc_copy(3).start()
        return mx

    lax.fori_loop(0, 12, tail, scores(0, kvt.at[1], blk(0)))

    def o_dst(e, yq):
        return dev(x, yq, 2 * c + e, s)

    def o_copy(e, yq):
        return rcopy(osend.at[e, yq], obuf.at[s, head], o_s, o_r.at[head], o_dst(e, yq))

    def keep_o(e, yq):
        obuf[s, head] = osend[e, yq]

    for e in range(2):
        b = blk(jnp.int32(HEADS - 2 + e))
        cc_copy(2 + e).wait_recv()
        merge(b, cb_core.at[2 + e])
        cy_copy(e).wait_recv()
        merge(b, cb_y.at[e])
        o = accs[b, ACC, :] / jnp.sum(accs[b, LROW, :], axis=0, keepdims=True)
        for yq in range(4):
            osend[e, yq] = o[:, yq * HD:(yq + 1) * HD].T.astype(BF16)
            unless(o_dst(e, yq) == me, lambda: o_copy(e, yq).start(), lambda: keep_o(e, yq))

    def od_copy(h):
        return rcopy(obuf.at[c, h], obuf.at[c, h], od_s, od_r, mate)

    for h in range(HEADS):
        src = dev(x, 2 * (h % 2) + c, h // 2, z // 2)
        unless(src == me, lambda: drain(obuf.at[c, h], o_r.at[h]))
        od_copy(h).start()

    def spread_o(tok, tau):
        for h in range(HEADS):
            for g in range(4):
                col = (h * 4 + g) * HD
                olhs[tok, col:col + HD] = obuf[tau, h, g * TOK:(g + 1) * TOK, :]

    spread_o(my_tok, c)
    drain(obuf.at[nc], od_r)
    spread_o(mate_tok, nc)

    def y_copy(n):
        cols = pl.ds(n * WCOLS, OTILES[n])
        dst = pl.ds(pl.multiple_of(c * OHALF, HD) + n * WCOLS, OTILES[n])
        return rcopy(ysend.at[mate_tok, cols], ybuf.at[:, dst], y_s, y_r, mate)

    for n in range(4):
        wide = OTILES[n]
        wo_copy(n).wait()
        acc = None
        for k in range(0, QCOLS, OSTEP):
            ks = pl.ds(k, OSTEP)
            d = jnp.dot(olhs[:, ks], wbuf[n, ks, :wide], preferred_element_type=F32)
            acc = d if acc is None else acc + d
        cols = pl.ds(n * WCOLS, wide)
        dst = pl.ds(pl.multiple_of(c * OHALF, HD) + n * WCOLS, wide)
        ysend[:, cols] = (xbuf[:, dst].astype(F32) + acc).astype(BF16)
        y_copy(n).start()
        ybuf[:, dst] = ysend[my_tok, cols]
    drain(ysend.at[my_tok], y_r)
    fin = pltpu.make_async_copy(ybuf, out_hbm, loc_sem.at[0])
    fin.start()

    x_ex.wait_send()
    drain(kvt.at[0, pl.ds(0, HEADS - 1)], kv1_s)
    drain(kvt.at[pl.ds(0, 3)], kvx_s)
    q_kept = c == src_core
    all_q = qbuf.at[0]
    unless(q_kept, lambda: drain(all_q, q_s), lambda: drain(qbuf.at[0, pl.ds(0, 15)], q_s))
    unless(q_kept, lambda: drain(newbuf.at[0], n_s), lambda: drain(newbuf.at[0, pl.ds(0, HEADS - 1)], n_s))
    drain(all_q, qd_s)
    drain(newbuf.at[pl.ds(0, 3)], nx_s)
    drain(cb_core, cc_s)
    drain(cb_y, cy_s)
    o_kept = jnp.logical_and(s == c, z // 2 == c)
    unless(o_kept, lambda: drain(obuf.at[0], o_s), lambda: drain(obuf.at[0, pl.ds(0, HEADS - 1)], o_s))
    drain(obuf.at[0], od_s)
    drain(ysend.at[mate_tok], y_s)
    fin.wait()


def solution(mesh):
    def local_step(x_loc, pos_loc, k_loc, v_loc, w_q, w_k, w_v, w_o):
        me = lax.axis_index("cp")
        p0 = pos_loc[0] - HALF * me
        row = jnp.arange(PAIR, dtype=jnp.int32)
        pos = p0 + rel_pos((me // 2) * 2 + row // TOK, row % TOK)
        inv_freq = jnp.power(F32(ROPE_BASE), -(jnp.arange(HD // 2, dtype=F32) * 2.0 / HD))
        ang = pos.astype(F32)[:, None] * inv_freq[None, :]
        vm = pltpu.VMEM
        anyspec = pl.BlockSpec(memory_space=pl.ANY)
        vspec = pl.BlockSpec(memory_space=pltpu.VMEM)
        one = ()
        dmas = ((3,), (8,), (2,), one, (8,), one, (4, 2), one, (4,), one, (4,),
                one, one, one, one, one, (4,), one, (2,), one, (8,), one, one, one, one)
        return pl.pallas_call(
            kernel,
            out_shape=jax.ShapeDtypeStruct((TOK, MODEL), BF16),
            in_specs=[anyspec, anyspec, anyspec, vspec, vspec, anyspec, anyspec, anyspec, anyspec],
            out_specs=anyspec,
            scratch_shapes=[
                vm((PAIR, MODEL), BF16),
                vm((2, CACHE, HEADS, HD), BF16),
                vm((HEADS, 2 * CACHE, HD), BF16),
                vm((4, 8, 2 * CACHE, HD), BF16),
                vm((4, 2 * CACHE, HD), BF16),
                vm((4, 8, PAIR, HD), BF16),
                vm((2, 16, HD, HD), BF16),
                vm((HEADS, HD, QB), BF16),
                vm((4, 2, HD, HD), BF16),
                vm((4, 2, PAIR, HD), BF16),
                vm((HEADS, STAT, QB), F32),
                vm((4, STAT, QB), F32),
                vm((2, STAT, QB), F32),
                vm((2, KT, QB), F32),
                vm((4, MODEL, WCOLS), BF16),
                vm((2, 4, HD, HD), BF16),
                vm((2, HEADS, HD, HD), BF16),
                vm((PAIR, QCOLS), BF16),
                vm((4, RC, HD), jnp.int32),
                vm((PAIR, OHALF), BF16),
                vm((TOK, MODEL), BF16),
            ] + [pltpu.SemaphoreType.DMA(n) for n in dmas],
            compiler_params=pltpu.CompilerParams(
                collective_id=0, has_side_effects=True, vmem_limit_bytes=67043328),
        )(x_loc, k_loc, v_loc, jnp.cos(ang), jnp.sin(ang), w_q, w_k, w_v, w_o)

    tok_spec = P(("data", "cp"), None)
    pos_spec = P(("data", "cp"))
    cache_spec = P(("data", "cp"), None, None)
    return jax.shard_map(local_step, mesh=mesh, in_specs=(tok_spec, pos_spec, cache_spec, cache_spec, P(), P(), P(), P()), out_specs=tok_spec, check_vma=False)
```

```python
import math

import jax
import jax.numpy as jnp
from jax import lax
from jax.experimental import pallas as pl
from jax.experimental.pallas import tpu as pltpu
from jax.sharding import PartitionSpec as P

ROPE_BASE = 500000.0
F32 = jnp.float32
BF16 = jnp.bfloat16
HD = 128
SUB = 8
HEADS = 8
TOK = 32
HALF = TOK // 2
PAIR = 2 * TOK
CACHE = 256
QB = 512
KT = 2048
KN = 1024
RC = 256
SCALE2 = (1.0 / math.sqrt(HD)) * math.log2(math.e)
MODEL = 5120
GRP = 512
WCOLS = GRP + 2 * HD
QCOLS = 4096
OHALF = MODEL // 2
KSTEP = 2560
OSTEP = 2048
OTILES = (WCOLS, WCOLS, WCOLS, CACHE)
LAST_POS = 4064
PIECES = (0, 4, 1, 3, 5, 7, 2, 6)
TILES = 0xFA5FA5
BLOCKS = 0xEEE444
NEG = float(jnp.finfo(jnp.float32).min)
ACC = slice(HD)
MROW = slice(HD, HD + SUB)
LROW = slice(HD + SUB, HD + 2 * SUB)
STAT = HD + 2 * SUB
KROWS = slice(CACHE)
VLO = slice(CACHE, CACHE + HD)
VHI = slice(CACHE + HD, 2 * CACHE)


def dev(x, y, z, c):
    return ((z * 4 + y) * 4 + x) * 2 + c


def rel_pos(d, t):
    return jnp.where(t < HALF, HALF * d + t, LAST_POS - HALF * d + t)


def rcopy(src, dst, ss, rs, d):
    return pltpu.make_async_remote_copy(
        src_ref=src, dst_ref=dst, send_sem=ss, recv_sem=rs, device_id={"cp": d},
        device_id_type=pl.DeviceIdType.MESH)


def drain(ref, sem):
    pltpu.make_async_copy(ref, ref, sem).wait()


def unless(cond, run, other=None):
    pl.when(jnp.logical_not(cond))(run)
    if other is not None:
        pl.when(cond)(other)


def kernel(
    x_hbm, k_hbm, v_hbm, cos_ref, sin_ref, wq, wk, wv, wo, out_hbm,
    xbuf, kraw, kvsrc, kvt, kvn, newbuf, qbuf, qt, qsend, nsend, accs, cb_core, cb_y, sbuf,
    wbuf, osend, obuf, olhs, kpos, ysend, ybuf,
    loc_sem, w_sem, x_sem, kv1_s, kv1_r, kvx_s, kvx_r, q_s, q_r, qd_s, qd_r,
    n_s, n_r, nx_s, nx_r, cc_s, cc_r, cy_s, cy_r, o_s, o_r, od_s, od_r, y_s, y_r,
):
    me = lax.axis_index("cp")
    c = lax.rem(me, 2)
    x = lax.rem(me // 2, 4)
    y = lax.rem(me // 8, 4)
    z = me // 32
    nc = 1 - c
    half_b = y // 2
    s = lax.rem(y, 2)
    head = 2 * z + half_b
    src_core = head // 4
    here = z * 4 + y
    mate = dev(x, y, z, nc)
    xr, xl, xo = (lax.rem(x + i, 4) for i in (1, 3, 2))
    my_tok = pl.ds(pl.multiple_of(c * TOK, TOK), TOK)
    mate_tok = pl.ds(pl.multiple_of(nc * TOK, TOK), TOK)

    def wcopies(i):
        h = 4 * c + i
        cols = pl.ds(pl.multiple_of(h * HD, HD), HD)
        return [
            pltpu.make_async_copy(wq.at[:, pl.ds(pl.multiple_of(h * GRP, GRP), GRP)], wbuf.at[i, :, pl.ds(0, GRP)], w_sem.at[i]),
            pltpu.make_async_copy(wk.at[:, cols], wbuf.at[i, :, pl.ds(GRP, HD)], w_sem.at[i]),
            pltpu.make_async_copy(wv.at[:, cols], wbuf.at[i, :, pl.ds(GRP + HD, HD)], w_sem.at[i]),
        ]

    def wo_copy(n):
        wide = OTILES[n]
        cols = pl.ds(pl.multiple_of(c * OHALF, HD) + n * WCOLS, wide)
        return pltpu.make_async_copy(wo.at[:, cols], wbuf.at[n, pl.ds(0, QCOLS), pl.ds(0, wide)], w_sem.at[4 + n])

    first = [
        pltpu.make_async_copy(k_hbm, kraw.at[0], loc_sem.at[0]),
        pltpu.make_async_copy(v_hbm, kraw.at[1], loc_sem.at[1]),
        pltpu.make_async_copy(x_hbm, xbuf.at[my_tok, :], loc_sem.at[2]),
    ]
    for cp in first:
        cp.start()

    barrier = pltpu.get_barrier_semaphore()

    def greet(d):
        pl.semaphore_signal(barrier, inc=1, device_id={"cp": d}, device_id_type=pl.DeviceIdType.MESH)

    greet(mate)
    for xx in (xr, xl, xo):
        greet(dev(xx, y, z, c))

    def greet_chip(i, _):
        for cc in range(2):
            pl.when(i != here)(lambda: greet(dev(x, lax.rem(i, 4), i // 4, cc)))
        return _

    lax.fori_loop(0, 16, greet_chip, 0)

    for cp in first:
        cp.wait()
    for i in range(4):
        for cp in wcopies(i):
            cp.start()
    for hb in range(2):
        rows = slice(hb * HD, (hb + 1) * HD)
        kh = pltpu.einshape("abc->bac", kraw[0, rows])
        vh = pltpu.einshape("abc->bac", kraw[1, rows])
        for h in range(HEADS):
            kvsrc[h, rows, :] = kh[h]
            kvsrc[h, (VLO, VHI)[hb], :] = vh[h].T
    kvt[0, 0] = kvsrc[head]

    accs[:, ACC, :] = jnp.zeros((HEADS, HD, QB), F32)
    accs[:, MROW, :] = jnp.full((HEADS, SUB, QB), NEG, F32)
    accs[:, LROW, :] = jnp.zeros((HEADS, SUB, QB), F32)
    for xs in range(4):
        row = lax.broadcasted_iota(jnp.int32, (RC, HD), 0)
        r = row // TOK
        zs = lax.rem(z + lax.rem(r, 4), 4)
        ys = jnp.where(r >= 4, 3 - y, y)
        kpos[xs] = rel_pos(dev((x, xl, xr, xo)[xs], ys, zs, c), lax.rem(row, TOK))

    pl.semaphore_wait(barrier, 34)

    x_ex = rcopy(xbuf.at[my_tok, :], xbuf.at[my_tok, :], x_sem.at[0], x_sem.at[1], mate)
    x_ex.start()

    def slot(xs, p):
        return kvt.at[p // 4 * 2 + xs // 2, xs % 2 * 4 + p % 4]

    def ring_send(p):
        rcopy(slot(0, p), slot(1, p), kvx_s, kvx_r.at[1, p // 4], dev(xr, y, z, c)).start()
        rcopy(slot(0, p), slot(2, p), kvx_s, kvx_r.at[2, p // 4], dev(xl, y, z, c)).start()

    def stage1_send(p):
        r = PIECES[p]
        zd = lax.rem(z + 4 - r % 4, 4)
        yd = 3 - y if r >= 4 else y
        rcopy(kvsrc.at[2 * zd + yd // 2], slot(0, p), kv1_s, kv1_r.at[p], dev(x, yd, zd, c)).start()

    def stage1_arrive(p):
        drain(slot(0, p), kv1_r.at[p])
        ring_send(p)

    def ring_wait(xs, half):
        drain(kvt.at[0, pl.ds(0, 4)], kvx_r.at[xs, half])

    def forward(src, p):
        to = xr if src == 1 else xl
        rcopy(slot(src, p), slot(3, p), kvx_s, kvx_r.at[3, p // 4], dev(to, y, z, c)).start()

    def ring_pass(src, half):
        ring_wait(src, half)
        for p in range(2):
            forward(src, 4 * half + 2 * src - 2 + p)

    for p in range(1, 6):
        stage1_send(p)
    ring_send(0)

    x_ex.wait_recv()

    def q_dst(i, ss, tau):
        h = 4 * c + i
        return dev(x, 2 * lax.rem(h, 2) + ss, h // 2, tau)

    def q_copy(i, ss, tau):
        return rcopy(qsend.at[i, tau], qbuf.at[tau, here], q_s, q_r.at[here // 4], q_dst(i, ss, tau))

    def n_dst(i):
        h = 4 * c + i
        zd = h // 2
        same = lax.rem(h, 2) == half_b
        return dev(x, jnp.where(same, y, 3 - y), zd, 0), jnp.where(same, 0, 4) + lax.rem(z + 4 - zd, 4)

    def n_copy(i, tau):
        d, r = n_dst(i)
        return rcopy(nsend.at[i, tau], newbuf.at[0, r], n_s, n_r, d + tau)

    cosv = jnp.concatenate([cos_ref[...]] * 2, axis=1)
    sinv = jnp.concatenate([-sin_ref[...], sin_ref[...]], axis=1)

    def rot(u):
        u = u.astype(F32)
        return (u * cosv + pltpu.roll(u, HD // 2, 1) * sinv).astype(BF16)

    for i in range(4):
        drain(wbuf.at[i], w_sem.at[i])
        acc = None
        for k in range(0, MODEL, KSTEP):
            ks = pl.ds(k, KSTEP)
            d = jnp.dot(xbuf[:, ks], wbuf[i, ks, :], preferred_element_type=F32)
            acc = d if acc is None else acc + d
        wo_copy(i).start()
        proj = acc.astype(BF16)
        for g in range(4):
            ro = rot(proj[:, g * HD:(g + 1) * HD])
            for tau in range(2):
                qsend[i, tau, g * TOK:(g + 1) * TOK, :] = ro[tau * TOK:(tau + 1) * TOK]
        kn = rot(proj[:, GRP:GRP + HD])
        vn = proj[:, GRP + HD:]
        for tau in range(2):
            rows = slice(tau * TOK, (tau + 1) * TOK)
            nsend[i, tau, :TOK, :] = kn[rows]
            nsend[i, tau, TOK:, :] = vn[rows]

        def keep_q(tau):
            qbuf[tau, here] = qsend[i, tau]

        def keep_n(tau):
            newbuf[0, 0] = nsend[i, tau]

        for tau in range(2):
            for ss in range(2):
                unless(q_dst(i, ss, tau) == me, lambda: q_copy(i, ss, tau).start(), lambda: keep_q(tau))
            unless(n_dst(i)[0] + tau == me, lambda: n_copy(i, tau).start(), lambda: keep_n(tau))
        for p in ((), (1, 2), (3,), ())[i]:
            stage1_arrive(p)

    for p in range(4, 6):
        stage1_arrive(p)

    def transpose_q(tau, zq):
        for yq in range(4):
            qt[tau * 4 + zq, :, yq * HD:(yq + 1) * HD] = qbuf[tau, zq * 4 + yq].T

    for zq in range(4):
        rows = pl.ds(zq * 4, 4)
        unless(jnp.logical_and(zq == z, c == src_core),
               lambda: drain(qbuf.at[c, rows], q_r.at[zq]),
               lambda: drain(qbuf.at[c, pl.ds(zq * 4, 3)], q_r.at[zq]))
        rcopy(qbuf.at[c, rows], qbuf.at[c, rows], qd_s, qd_r.at[zq], mate).start()
        transpose_q(c, zq)

    unless(c == src_core, lambda: drain(newbuf.at[0], n_r), lambda: drain(newbuf.at[0, pl.ds(1, HEADS - 1)], n_r))
    for k, xx in enumerate((xr, xl, xo)):
        rcopy(newbuf.at[0], newbuf.at[k + 1], nx_s, nx_r, dev(xx, y, z, c)).start()

    for p in range(6, HEADS):
        stage1_send(p)
    ring_pass(1, 0)
    ring_pass(2, 0)

    for zq in range(4):
        drain(qbuf.at[nc, pl.ds(zq * 4, 4)], qd_r.at[zq])
        transpose_q(nc, zq)

    def fold(op, v):
        return op(v.reshape(RC // SUB, SUB, QB), axis=0)

    def spread(v):
        return v.reshape(-1, SUB, QB)

    def q_pos(qb):
        lane = lax.broadcasted_iota(jnp.int32, (SUB, QB), 1)
        return rel_pos(dev(x, lane // HD, lax.rem(qb, 4), qb // 4), lax.rem(lane, TOK))

    def score_chunk(par, ref, qb, ch, mx, masked):
        sc = jnp.dot(ref[ch, KROWS, :], qt[qb], preferred_element_type=F32)
        if masked:
            kp = spread(jnp.concatenate([kpos[ch]] * (QB // HD), axis=1))
            sc = jnp.where(kp <= q_pos(qb)[None], spread(sc), -jnp.inf).reshape(RC, QB)
        sbuf[par, pl.ds(ch * RC, RC), :] = sc
        f = fold(jnp.max, sc)
        return f if mx is None else jnp.maximum(mx, f)

    def scores(par, ref, qb, masked=False):
        mx = None
        for ch in range(ref.shape[0]):
            mx = score_chunk(par, ref, qb, ch, mx, masked)
        return mx

    def step(par, mx, ref, qb, nref, nqb, masked=False):
        m_old = accs[qb, MROW, :]
        mn = jnp.maximum(m_old, jnp.broadcast_to(jnp.max(mx, axis=0, keepdims=True), (SUB, QB)))
        a = jnp.exp2((m_old - mn) * SCALE2)
        mx2 = ls = pv = None
        for ch in range(ref.shape[0]):
            mx2 = score_chunk(1 - par, nref, nqb, ch, mx2, masked)
            p = jnp.exp2((spread(sbuf[par, pl.ds(ch * RC, RC), :]) - mn[None]) * SCALE2)
            f = jnp.sum(p, axis=0)
            ls = f if ls is None else ls + f
            vt = jnp.concatenate([ref[ch, VLO, :], ref[ch, VHI, :]], axis=1)
            d = jnp.dot(vt, p.reshape(RC, QB).astype(BF16), preferred_element_type=F32)
            pv = d if pv is None else pv + d
        accs[qb, ACC, :] = (spread(accs[qb, ACC, :]) * a[None]).reshape(HD, QB) + pv
        accs[qb, MROW, :] = mn
        accs[qb, LROW, :] = accs[qb, LROW, :] * a + ls
        return mx2

    def tile_pass(ref, masked=False, beside=()):
        def body(it, mx):
            qb = 2 * it
            mx = step(0, mx, ref, qb, ref, qb + 1, masked)
            mx = step(1, mx, ref, qb + 1, ref, lax.rem(qb + 2, HEADS), masked)
            for k, run in enumerate(beside):
                pl.when(it == k)(run)
            return mx

        lax.fori_loop(0, HEADS // 2, body, scores(0, ref, 0, masked))

    def nothing():
        pass

    def arrive(p):
        return lambda: stage1_arrive(p)

    tile_pass(kvt.at[0], beside=(nothing, nothing, arrive(6), arrive(7)))

    drain(newbuf.at[pl.ds(1, 3)], nx_r)
    for xs in range(4):
        for r in range(HEADS):
            kvn[xs, r * TOK:(r + 1) * TOK, :] = newbuf[xs, r, :TOK, :]
        for hf in range(2):
            vblk = jnp.concatenate([newbuf[xs, hf * 4 + r, TOK:, :] for r in range(4)], axis=0)
            kvn[xs, (VLO, VHI)[hf], :] = vblk.T

    tile_pass(kvn, True)

    ring_wait(3, 0)

    def blk(u):
        cc = jnp.where(lax.rem(u // 2, 2) == 0, nc, c)
        return 4 * jnp.where(u < 4, 1 - s, s) + 2 * cc + lax.rem(u, 2)

    def cc_copy(k):
        return rcopy(accs.at[blk(k + k // 2 * 2)], cb_core.at[k], cc_s, cc_r.at[k], mate)

    y_mate = dev(x, 2 * half_b + 1 - s, z, c)

    def cy_copy(k):
        return rcopy(accs.at[blk(k + 2)], cb_y.at[k], cy_s, cy_r.at[k], y_mate)

    def merge(dst, src):
        m0, m1 = accs[dst, MROW, :], src[MROW, :]
        mn = jnp.maximum(m0, m1)
        e0, e1 = jnp.exp2((m0 - mn) * SCALE2), jnp.exp2((m1 - mn) * SCALE2)
        accs[dst, ACC, :] = (spread(accs[dst, ACC, :]) * e0[None] + spread(src[ACC, :]) * e1[None]).reshape(HD, QB)
        accs[dst, MROW, :] = mn
        accs[dst, LROW, :] = accs[dst, LROW, :] * e0 + src[LROW, :] * e1

    def tail(it, mx):
        @pl.when(it == 0)
        def _():
            ring_pass(1, 1)
            ring_pass(2, 1)

        pl.when(it == 3)(lambda: ring_wait(3, 1))

        def at(i):
            return jnp.bitwise_and(TILES >> (2 * i), 3), 2 * jnp.bitwise_and(BLOCKS >> (2 * i), 3)

        k0, u0 = at(it)
        k1, u1 = at(jnp.minimum(it + 1, 11))
        mx = step(0, mx, kvt.at[k0], blk(u0), kvt.at[k0], blk(u0 + 1))
        mx = step(1, mx, kvt.at[k0], blk(u0 + 1), kvt.at[k1], blk(u1))

        @pl.when(it == 4)
        def _():
            cc_copy(0).start()
            cc_copy(1).start()

        @pl.when(it == 5)
        def _():
            for k in range(2):
                cc_copy(k).wait_recv()
                merge(blk(2 + k), cb_core.at[k])
                cy_copy(k).start()

        @pl.when(it == 10)
        def _():
            cc_copy(2).start()
            cc_copy(3).start()
        return mx

    lax.fori_loop(0, 12, tail, scores(0, kvt.at[1], blk(0)))

    def o_dst(e, yq):
        return dev(x, yq, 2 * c + e, s)

    def o_copy(e, yq):
        return rcopy(osend.at[e, yq], obuf.at[s, head], o_s, o_r.at[head], o_dst(e, yq))

    def keep_o(e, yq):
        obuf[s, head] = osend[e, yq]

    for e in range(2):
        b = blk(jnp.int32(HEADS - 2 + e))
        cc_copy(2 + e).wait_recv()
        merge(b, cb_core.at[2 + e])
        cy_copy(e).wait_recv()
        merge(b, cb_y.at[e])
        o = accs[b, ACC, :] / jnp.sum(accs[b, LROW, :], axis=0, keepdims=True)
        for yq in range(4):
            osend[e, yq] = o[:, yq * HD:(yq + 1) * HD].T.astype(BF16)
            unless(o_dst(e, yq) == me, lambda: o_copy(e, yq).start(), lambda: keep_o(e, yq))

    def od_copy(h):
        return rcopy(obuf.at[c, h], obuf.at[c, h], od_s, od_r, mate)

    for h in range(HEADS):
        src = dev(x, 2 * (h % 2) + c, h // 2, z // 2)
        unless(src == me, lambda: drain(obuf.at[c, h], o_r.at[h]))
        od_copy(h).start()

    def spread_o(tok, tau):
        for h in range(HEADS):
            for g in range(4):
                col = (h * 4 + g) * HD
                olhs[tok, col:col + HD] = obuf[tau, h, g * TOK:(g + 1) * TOK, :]

    spread_o(my_tok, c)
    drain(obuf.at[nc], od_r)
    spread_o(mate_tok, nc)

    def y_copy(n):
        cols = pl.ds(n * WCOLS, OTILES[n])
        dst = pl.ds(pl.multiple_of(c * OHALF, HD) + n * WCOLS, OTILES[n])
        return rcopy(ysend.at[mate_tok, cols], ybuf.at[:, dst], y_s, y_r, mate)

    for n in range(4):
        wide = OTILES[n]
        wo_copy(n).wait()
        acc = None
        for k in range(0, QCOLS, OSTEP):
            ks = pl.ds(k, OSTEP)
            d = jnp.dot(olhs[:, ks], wbuf[n, ks, :wide], preferred_element_type=F32)
            acc = d if acc is None else acc + d
        cols = pl.ds(n * WCOLS, wide)
        dst = pl.ds(pl.multiple_of(c * OHALF, HD) + n * WCOLS, wide)
        ysend[:, cols] = (xbuf[:, dst].astype(F32) + acc).astype(BF16)
        y_copy(n).start()
        ybuf[:, dst] = ysend[my_tok, cols]
    drain(ysend.at[my_tok], y_r)
    fin = pltpu.make_async_copy(ybuf, out_hbm, loc_sem.at[0])
    fin.start()

    x_ex.wait_send()
    drain(kvt.at[0, pl.ds(0, HEADS - 1)], kv1_s)
    drain(kvt.at[pl.ds(0, 3)], kvx_s)
    q_kept = c == src_core
    all_q = qbuf.at[0]
    unless(q_kept, lambda: drain(all_q, q_s), lambda: drain(qbuf.at[0, pl.ds(0, 15)], q_s))
    unless(q_kept, lambda: drain(newbuf.at[0], n_s), lambda: drain(newbuf.at[0, pl.ds(0, HEADS - 1)], n_s))
    drain(all_q, qd_s)
    drain(newbuf.at[pl.ds(0, 3)], nx_s)
    drain(cb_core, cc_s)
    drain(cb_y, cy_s)
    o_kept = jnp.logical_and(s == c, z // 2 == c)
    unless(o_kept, lambda: drain(obuf.at[0], o_s), lambda: drain(obuf.at[0, pl.ds(0, HEADS - 1)], o_s))
    drain(obuf.at[0], od_s)
    drain(ysend.at[mate_tok], y_s)
    fin.wait()


def solution(mesh):
    def local_step(x_loc, pos_loc, k_loc, v_loc, w_q, w_k, w_v, w_o):
        me = lax.axis_index("cp")
        p0 = pos_loc[0] - HALF * me
        row = jnp.arange(PAIR, dtype=jnp.int32)
        pos = p0 + rel_pos((me // 2) * 2 + row // TOK, row % TOK)
        inv_freq = jnp.power(F32(ROPE_BASE), -(jnp.arange(HD // 2, dtype=F32) * 2.0 / HD))
        ang = pos.astype(F32)[:, None] * inv_freq[None, :]
        vm = pltpu.VMEM
        anyspec = pl.BlockSpec(memory_space=pl.ANY)
        vspec = pl.BlockSpec(memory_space=pltpu.VMEM)
        one = ()
        dmas = ((3,), (8,), (2,), one, (8,), one, (4, 2), one, (4,), one, (4,),
                one, one, one, one, one, (4,), one, (2,), one, (8,), one, one, one, one)
        return pl.pallas_call(
            kernel,
            out_shape=jax.ShapeDtypeStruct((TOK, MODEL), BF16),
            in_specs=[anyspec, anyspec, anyspec, vspec, vspec, anyspec, anyspec, anyspec, anyspec],
            out_specs=anyspec,
            scratch_shapes=[
                vm((PAIR, MODEL), BF16),
                vm((2, CACHE, HEADS, HD), BF16),
                vm((HEADS, 2 * CACHE, HD), BF16),
                vm((4, 8, 2 * CACHE, HD), BF16),
                vm((4, 2 * CACHE, HD), BF16),
                vm((4, 8, PAIR, HD), BF16),
                vm((2, 16, HD, HD), BF16),
                vm((HEADS, HD, QB), BF16),
                vm((4, 2, HD, HD), BF16),
                vm((4, 2, PAIR, HD), BF16),
                vm((HEADS, STAT, QB), F32),
                vm((4, STAT, QB), F32),
                vm((2, STAT, QB), F32),
                vm((2, KT, QB), F32),
                vm((4, MODEL, WCOLS), BF16),
                vm((2, 4, HD, HD), BF16),
                vm((2, HEADS, HD, HD), BF16),
                vm((PAIR, QCOLS), BF16),
                vm((4, RC, HD), jnp.int32),
                vm((PAIR, OHALF), BF16),
                vm((TOK, MODEL), BF16),
            ] + [pltpu.SemaphoreType.DMA(n) for n in dmas],
            compiler_params=pltpu.CompilerParams(
                collective_id=0, has_side_effects=True, vmem_limit_bytes=67043328),
        )(x_loc, k_loc, v_loc, jnp.cos(ang), jnp.sin(ang), w_q, w_k, w_v, w_o)

    tok_spec = P(("data", "cp"), None)
    pos_spec = P(("data", "cp"))
    cache_spec = P(("data", "cp"), None, None)
    return jax.shard_map(local_step, mesh=mesh, in_specs=(tok_spec, pos_spec, cache_spec, cache_spec, P(), P(), P(), P()), out_specs=tok_spec, check_vma=False)
```

```python
import math

import jax
import jax.numpy as jnp
from jax import lax
from jax.experimental import pallas as pl
from jax.experimental.pallas import tpu as pltpu
from jax.sharding import PartitionSpec as P

ROPE_BASE = 500000.0
F32 = jnp.float32
BF16 = jnp.bfloat16
HD = 128
SUB = 8
HEADS = 8
TOK = 32
HALF = TOK // 2
PAIR = 2 * TOK
CACHE = 256
QB = 512
KT = 2048
KN = 1024
RC = 256
SCALE2 = (1.0 / math.sqrt(HD)) * math.log2(math.e)
MODEL = 5120
GRP = 512
WCOLS = GRP + 2 * HD
QCOLS = 4096
OHALF = MODEL // 2
KSTEP = 2560
OSTEP = 2048
OTILES = (WCOLS, WCOLS, WCOLS, CACHE)
LAST_POS = 4064
PIECES = (0, 4, 1, 3, 5, 7, 2, 6)
TILES = 0xFA5FA5
BLOCKS = 0xEEE444
NEG = float(jnp.finfo(jnp.float32).min)
ACC = slice(HD)
MROW = slice(HD, HD + SUB)
LROW = slice(HD + SUB, HD + 2 * SUB)
STAT = HD + 2 * SUB
KROWS = slice(CACHE)
VLO = slice(CACHE, CACHE + HD)
VHI = slice(CACHE + HD, 2 * CACHE)


def dev(x, y, z, c):
    return ((z * 4 + y) * 4 + x) * 2 + c


def rel_pos(d, t):
    return jnp.where(t < HALF, HALF * d + t, LAST_POS - HALF * d + t)


def rcopy(src, dst, ss, rs, d):
    return pltpu.make_async_remote_copy(
        src_ref=src, dst_ref=dst, send_sem=ss, recv_sem=rs, device_id={"cp": d},
        device_id_type=pl.DeviceIdType.MESH)


def drain(ref, sem):
    pltpu.make_async_copy(ref, ref, sem).wait()


def unless(cond, run, other=None):
    pl.when(jnp.logical_not(cond))(run)
    if other is not None:
        pl.when(cond)(other)


def kernel(
    x_hbm, k_hbm, v_hbm, cos_ref, sin_ref, wq, wk, wv, wo, out_hbm,
    xbuf, kraw, kvsrc, kvt, kvn, newbuf, qbuf, qt, qsend, nsend, accs, cb_core, cb_y, sbuf,
    wbuf, osend, obuf, olhs, kpos, ysend, ybuf,
    loc_sem, w_sem, x_sem, kv1_s, kv1_r, kvx_s, kvx_r, q_s, q_r, qd_s, qd_r,
    n_s, n_r, nx_s, nx_r, cc_s, cc_r, cy_s, cy_r, o_s, o_r, od_s, od_r, y_s, y_r,
):
    me = lax.axis_index("cp")
    c = lax.rem(me, 2)
    x = lax.rem(me // 2, 4)
    y = lax.rem(me // 8, 4)
    z = me // 32
    nc = 1 - c
    half_b = y // 2
    s = lax.rem(y, 2)
    head = 2 * z + half_b
    src_core = head // 4
    here = z * 4 + y
    mate = dev(x, y, z, nc)
    xr, xl, xo = (lax.rem(x + i, 4) for i in (1, 3, 2))
    my_tok = pl.ds(pl.multiple_of(c * TOK, TOK), TOK)
    mate_tok = pl.ds(pl.multiple_of(nc * TOK, TOK), TOK)

    def wcopies(i):
        h = 4 * c + i
        cols = pl.ds(pl.multiple_of(h * HD, HD), HD)
        return [
            pltpu.make_async_copy(wq.at[:, pl.ds(pl.multiple_of(h * GRP, GRP), GRP)], wbuf.at[i, :, pl.ds(0, GRP)], w_sem.at[i]),
            pltpu.make_async_copy(wk.at[:, cols], wbuf.at[i, :, pl.ds(GRP, HD)], w_sem.at[i]),
            pltpu.make_async_copy(wv.at[:, cols], wbuf.at[i, :, pl.ds(GRP + HD, HD)], w_sem.at[i]),
        ]

    def wo_copy(n):
        wide = OTILES[n]
        cols = pl.ds(pl.multiple_of(c * OHALF, HD) + n * WCOLS, wide)
        return pltpu.make_async_copy(wo.at[:, cols], wbuf.at[n, pl.ds(0, QCOLS), pl.ds(0, wide)], w_sem.at[4 + n])

    first = [
        pltpu.make_async_copy(k_hbm, kraw.at[0], loc_sem.at[0]),
        pltpu.make_async_copy(v_hbm, kraw.at[1], loc_sem.at[1]),
        pltpu.make_async_copy(x_hbm, xbuf.at[my_tok, :], loc_sem.at[2]),
    ]
    for cp in first:
        cp.start()

    barrier = pltpu.get_barrier_semaphore()

    def greet(d):
        pl.semaphore_signal(barrier, inc=1, device_id={"cp": d}, device_id_type=pl.DeviceIdType.MESH)

    greet(mate)
    for xx in (xr, xl, xo):
        greet(dev(xx, y, z, c))

    def greet_chip(i, _):
        for cc in range(2):
            pl.when(i != here)(lambda: greet(dev(x, lax.rem(i, 4), i // 4, cc)))
        return _

    lax.fori_loop(0, 16, greet_chip, 0)

    for cp in first:
        cp.wait()
    for i in range(4):
        for cp in wcopies(i):
            cp.start()
    for hb in range(2):
        rows = slice(hb * HD, (hb + 1) * HD)
        kh = pltpu.einshape("abc->bac", kraw[0, rows])
        vh = pltpu.einshape("abc->bac", kraw[1, rows])
        for h in range(HEADS):
            kvsrc[h, rows, :] = kh[h]
            kvsrc[h, (VLO, VHI)[hb], :] = vh[h].T
    kvt[0, 0] = kvsrc[head]

    accs[:, ACC, :] = jnp.zeros((HEADS, HD, QB), F32)
    accs[:, MROW, :] = jnp.full((HEADS, SUB, QB), NEG, F32)
    accs[:, LROW, :] = jnp.zeros((HEADS, SUB, QB), F32)
    for xs in range(4):
        row = lax.broadcasted_iota(jnp.int32, (RC, HD), 0)
        r = row // TOK
        zs = lax.rem(z + lax.rem(r, 4), 4)
        ys = jnp.where(r >= 4, 3 - y, y)
        kpos[xs] = rel_pos(dev((x, xl, xr, xo)[xs], ys, zs, c), lax.rem(row, TOK))

    pl.semaphore_wait(barrier, 34)

    x_ex = rcopy(xbuf.at[my_tok, :], xbuf.at[my_tok, :], x_sem.at[0], x_sem.at[1], mate)
    x_ex.start()

    def slot(xs, p):
        return kvt.at[p // 4 * 2 + xs // 2, xs % 2 * 4 + p % 4]

    def ring_send(p):
        rcopy(slot(0, p), slot(1, p), kvx_s, kvx_r.at[1, p // 4], dev(xr, y, z, c)).start()
        rcopy(slot(0, p), slot(2, p), kvx_s, kvx_r.at[2, p // 4], dev(xl, y, z, c)).start()

    def stage1_send(p):
        r = PIECES[p]
        zd = lax.rem(z + 4 - r % 4, 4)
        yd = 3 - y if r >= 4 else y
        rcopy(kvsrc.at[2 * zd + yd // 2], slot(0, p), kv1_s, kv1_r.at[p], dev(x, yd, zd, c)).start()

    def stage1_arrive(p):
        drain(slot(0, p), kv1_r.at[p])
        ring_send(p)

    def ring_wait(xs, half):
        drain(kvt.at[0, pl.ds(0, 4)], kvx_r.at[xs, half])

    def forward(src, p):
        to = xr if src == 1 else xl
        rcopy(slot(src, p), slot(3, p), kvx_s, kvx_r.at[3, p // 4], dev(to, y, z, c)).start()

    def ring_pass(src, half):
        ring_wait(src, half)
        for p in range(2):
            forward(src, 4 * half + 2 * src - 2 + p)

    for p in range(1, 6):
        stage1_send(p)
    ring_send(0)

    x_ex.wait_recv()

    def q_dst(i, ss, tau):
        h = 4 * c + i
        return dev(x, 2 * lax.rem(h, 2) + ss, h // 2, tau)

    def q_copy(i, ss, tau):
        return rcopy(qsend.at[i, tau], qbuf.at[tau, here], q_s, q_r.at[here // 4], q_dst(i, ss, tau))

    def n_dst(i):
        h = 4 * c + i
        zd = h // 2
        same = lax.rem(h, 2) == half_b
        return dev(x, jnp.where(same, y, 3 - y), zd, 0), jnp.where(same, 0, 4) + lax.rem(z + 4 - zd, 4)

    def n_copy(i, tau):
        d, r = n_dst(i)
        return rcopy(nsend.at[i, tau], newbuf.at[0, r], n_s, n_r, d + tau)

    cosv = jnp.concatenate([cos_ref[...]] * 2, axis=1)
    sinv = jnp.concatenate([-sin_ref[...], sin_ref[...]], axis=1)

    def rot(u):
        u = u.astype(F32)
        return (u * cosv + pltpu.roll(u, HD // 2, 1) * sinv).astype(BF16)

    for i in range(4):
        drain(wbuf.at[i], w_sem.at[i])
        acc = None
        for k in range(0, MODEL, KSTEP):
            ks = pl.ds(k, KSTEP)
            d = jnp.dot(xbuf[:, ks], wbuf[i, ks, :], preferred_element_type=F32)
            acc = d if acc is None else acc + d
        wo_copy(i).start()
        proj = acc.astype(BF16)
        for g in range(4):
            ro = rot(proj[:, g * HD:(g + 1) * HD])
            for tau in range(2):
                qsend[i, tau, g * TOK:(g + 1) * TOK, :] = ro[tau * TOK:(tau + 1) * TOK]
        kn = rot(proj[:, GRP:GRP + HD])
        vn = proj[:, GRP + HD:]
        for tau in range(2):
            rows = slice(tau * TOK, (tau + 1) * TOK)
            nsend[i, tau, :TOK, :] = kn[rows]
            nsend[i, tau, TOK:, :] = vn[rows]

        def keep_q(tau):
            qbuf[tau, here] = qsend[i, tau]

        def keep_n(tau):
            newbuf[0, 0] = nsend[i, tau]

        for tau in range(2):
            for ss in range(2):
                unless(q_dst(i, ss, tau) == me, lambda: q_copy(i, ss, tau).start(), lambda: keep_q(tau))
            unless(n_dst(i)[0] + tau == me, lambda: n_copy(i, tau).start(), lambda: keep_n(tau))
        for p in ((), (1, 2), (3,), ())[i]:
            stage1_arrive(p)

    for p in range(4, 6):
        stage1_arrive(p)

    def transpose_q(tau, zq):
        for yq in range(4):
            qt[tau * 4 + zq, :, yq * HD:(yq + 1) * HD] = qbuf[tau, zq * 4 + yq].T

    for zq in range(4):
        rows = pl.ds(zq * 4, 4)
        unless(jnp.logical_and(zq == z, c == src_core),
               lambda: drain(qbuf.at[c, rows], q_r.at[zq]),
               lambda: drain(qbuf.at[c, pl.ds(zq * 4, 3)], q_r.at[zq]))
        rcopy(qbuf.at[c, rows], qbuf.at[c, rows], qd_s, qd_r.at[zq], mate).start()
        transpose_q(c, zq)

    unless(c == src_core, lambda: drain(newbuf.at[0], n_r), lambda: drain(newbuf.at[0, pl.ds(1, HEADS - 1)], n_r))
    for k, xx in enumerate((xr, xl, xo)):
        rcopy(newbuf.at[0], newbuf.at[k + 1], nx_s, nx_r, dev(xx, y, z, c)).start()

    for p in range(6, HEADS):
        stage1_send(p)
    ring_pass(1, 0)
    ring_pass(2, 0)

    def mate_queries():
        for zq in range(4):
            drain(qbuf.at[nc, pl.ds(zq * 4, 4)], qd_r.at[zq])
            transpose_q(nc, zq)

    def fold(op, v):
        return op(v.reshape(RC // SUB, SUB, QB), axis=0)

    def spread(v):
        return v.reshape(-1, SUB, QB)

    def q_pos(qb):
        lane = lax.broadcasted_iota(jnp.int32, (SUB, QB), 1)
        return rel_pos(dev(x, lane // HD, lax.rem(qb, 4), qb // 4), lax.rem(lane, TOK))

    def score_chunk(par, ref, qb, ch, mx, masked):
        sc = jnp.dot(ref[ch, KROWS, :], qt[qb], preferred_element_type=F32)
        if masked:
            kp = spread(jnp.concatenate([kpos[ch]] * (QB // HD), axis=1))
            sc = jnp.where(kp <= q_pos(qb)[None], spread(sc), -jnp.inf).reshape(RC, QB)
        sbuf[par, pl.ds(ch * RC, RC), :] = sc
        f = fold(jnp.max, sc)
        return f if mx is None else jnp.maximum(mx, f)

    def scores(par, ref, qb, masked=False):
        mx = None
        for ch in range(ref.shape[0]):
            mx = score_chunk(par, ref, qb, ch, mx, masked)
        return mx

    def step(par, mx, ref, qb, nref, nqb, masked=False):
        m_old = accs[qb, MROW, :]
        mn = jnp.maximum(m_old, jnp.broadcast_to(jnp.max(mx, axis=0, keepdims=True), (SUB, QB)))
        a = jnp.exp2((m_old - mn) * SCALE2)
        mx2 = ls = pv = None
        for ch in range(ref.shape[0]):
            mx2 = score_chunk(1 - par, nref, nqb, ch, mx2, masked)
            p = jnp.exp2((spread(sbuf[par, pl.ds(ch * RC, RC), :]) - mn[None]) * SCALE2)
            f = jnp.sum(p, axis=0)
            ls = f if ls is None else ls + f
            vt = jnp.concatenate([ref[ch, VLO, :], ref[ch, VHI, :]], axis=1)
            d = jnp.dot(vt, p.reshape(RC, QB).astype(BF16), preferred_element_type=F32)
            pv = d if pv is None else pv + d
        accs[qb, ACC, :] = (spread(accs[qb, ACC, :]) * a[None]).reshape(HD, QB) + pv
        accs[qb, MROW, :] = mn
        accs[qb, LROW, :] = accs[qb, LROW, :] * a + ls
        return mx2

    def tile_pass(ref, masked=False, beside=()):
        def body(it, mx):
            qb, q1, q2 = (lax.rem(2 * it + 4 * c + k, HEADS) for k in range(3))
            mx = step(0, mx, ref, qb, ref, q1, masked)
            mx = step(1, mx, ref, q1, ref, q2, masked)
            for k, run in enumerate(beside):
                pl.when(it == k)(run)
            return mx

        lax.fori_loop(0, HEADS // 2, body, scores(0, ref, 4 * c, masked))

    def nothing():
        pass

    def arrive(p):
        return lambda: stage1_arrive(p)

    tile_pass(kvt.at[0], beside=(mate_queries, nothing, arrive(6), arrive(7)))

    drain(newbuf.at[pl.ds(1, 3)], nx_r)
    for xs in range(4):
        for r in range(HEADS):
            kvn[xs, r * TOK:(r + 1) * TOK, :] = newbuf[xs, r, :TOK, :]
        for hf in range(2):
            vblk = jnp.concatenate([newbuf[xs, hf * 4 + r, TOK:, :] for r in range(4)], axis=0)
            kvn[xs, (VLO, VHI)[hf], :] = vblk.T

    tile_pass(kvn, True)

    ring_wait(3, 0)

    def blk(u):
        cc = jnp.where(lax.rem(u // 2, 2) == 0, nc, c)
        return 4 * jnp.where(u < 4, 1 - s, s) + 2 * cc + lax.rem(u, 2)

    def cc_copy(k):
        return rcopy(accs.at[blk(k + k // 2 * 2)], cb_core.at[k], cc_s, cc_r.at[k], mate)

    y_mate = dev(x, 2 * half_b + 1 - s, z, c)

    def cy_copy(k):
        return rcopy(accs.at[blk(k + 2)], cb_y.at[k], cy_s, cy_r.at[k], y_mate)

    def merge(dst, src):
        m0, m1 = accs[dst, MROW, :], src[MROW, :]
        mn = jnp.maximum(m0, m1)
        e0, e1 = jnp.exp2((m0 - mn) * SCALE2), jnp.exp2((m1 - mn) * SCALE2)
        accs[dst, ACC, :] = (spread(accs[dst, ACC, :]) * e0[None] + spread(src[ACC, :]) * e1[None]).reshape(HD, QB)
        accs[dst, MROW, :] = mn
        accs[dst, LROW, :] = accs[dst, LROW, :] * e0 + src[LROW, :] * e1

    def tail(it, mx):
        @pl.when(it == 0)
        def _():
            ring_pass(1, 1)
            ring_pass(2, 1)

        pl.when(it == 3)(lambda: ring_wait(3, 1))

        def at(i):
            return jnp.bitwise_and(TILES >> (2 * i), 3), 2 * jnp.bitwise_and(BLOCKS >> (2 * i), 3)

        k0, u0 = at(it)
        k1, u1 = at(jnp.minimum(it + 1, 11))
        mx = step(0, mx, kvt.at[k0], blk(u0), kvt.at[k0], blk(u0 + 1))
        mx = step(1, mx, kvt.at[k0], blk(u0 + 1), kvt.at[k1], blk(u1))

        @pl.when(it == 4)
        def _():
            cc_copy(0).start()
            cc_copy(1).start()

        @pl.when(it == 5)
        def _():
            for k in range(2):
                cc_copy(k).wait_recv()
                merge(blk(2 + k), cb_core.at[k])
                cy_copy(k).start()

        @pl.when(it == 10)
        def _():
            cc_copy(2).start()
            cc_copy(3).start()
        return mx

    lax.fori_loop(0, 12, tail, scores(0, kvt.at[1], blk(0)))

    def o_dst(e, yq):
        return dev(x, yq, 2 * c + e, s)

    def o_copy(e, yq):
        return rcopy(osend.at[e, yq], obuf.at[s, head], o_s, o_r.at[head], o_dst(e, yq))

    def keep_o(e, yq):
        obuf[s, head] = osend[e, yq]

    for e in range(2):
        b = blk(jnp.int32(HEADS - 2 + e))
        cc_copy(2 + e).wait_recv()
        merge(b, cb_core.at[2 + e])
        cy_copy(e).wait_recv()
        merge(b, cb_y.at[e])
        o = accs[b, ACC, :] / jnp.sum(accs[b, LROW, :], axis=0, keepdims=True)
        for yq in range(4):
            osend[e, yq] = o[:, yq * HD:(yq + 1) * HD].T.astype(BF16)
            unless(o_dst(e, yq) == me, lambda: o_copy(e, yq).start(), lambda: keep_o(e, yq))

    def od_copy(h):
        return rcopy(obuf.at[c, h], obuf.at[c, h], od_s, od_r, mate)

    for h in range(HEADS):
        src = dev(x, 2 * (h % 2) + c, h // 2, z // 2)
        unless(src == me, lambda: drain(obuf.at[c, h], o_r.at[h]))
        od_copy(h).start()

    def spread_o(tok, tau):
        for h in range(HEADS):
            for g in range(4):
                col = (h * 4 + g) * HD
                olhs[tok, col:col + HD] = obuf[tau, h, g * TOK:(g + 1) * TOK, :]

    spread_o(my_tok, c)
    drain(obuf.at[nc], od_r)
    spread_o(mate_tok, nc)

    def y_copy(n):
        cols = pl.ds(n * WCOLS, OTILES[n])
        dst = pl.ds(pl.multiple_of(c * OHALF, HD) + n * WCOLS, OTILES[n])
        return rcopy(ysend.at[mate_tok, cols], ybuf.at[:, dst], y_s, y_r, mate)

    for n in range(4):
        wide = OTILES[n]
        wo_copy(n).wait()
        acc = None
        for k in range(0, QCOLS, OSTEP):
            ks = pl.ds(k, OSTEP)
            d = jnp.dot(olhs[:, ks], wbuf[n, ks, :wide], preferred_element_type=F32)
            acc = d if acc is None else acc + d
        cols = pl.ds(n * WCOLS, wide)
        dst = pl.ds(pl.multiple_of(c * OHALF, HD) + n * WCOLS, wide)
        ysend[:, cols] = (xbuf[:, dst].astype(F32) + acc).astype(BF16)
        y_copy(n).start()
        ybuf[:, dst] = ysend[my_tok, cols]
    drain(ysend.at[my_tok], y_r)
    fin = pltpu.make_async_copy(ybuf, out_hbm, loc_sem.at[0])
    fin.start()

    x_ex.wait_send()
    drain(kvt.at[0, pl.ds(0, HEADS - 1)], kv1_s)
    drain(kvt.at[pl.ds(0, 3)], kvx_s)
    q_kept = c == src_core
    all_q = qbuf.at[0]
    unless(q_kept, lambda: drain(all_q, q_s), lambda: drain(qbuf.at[0, pl.ds(0, 15)], q_s))
    unless(q_kept, lambda: drain(newbuf.at[0], n_s), lambda: drain(newbuf.at[0, pl.ds(0, HEADS - 1)], n_s))
    drain(all_q, qd_s)
    drain(newbuf.at[pl.ds(0, 3)], nx_s)
    drain(cb_core, cc_s)
    drain(cb_y, cy_s)
    o_kept = jnp.logical_and(s == c, z // 2 == c)
    unless(o_kept, lambda: drain(obuf.at[0], o_s), lambda: drain(obuf.at[0, pl.ds(0, HEADS - 1)], o_s))
    drain(obuf.at[0], od_s)
    drain(ysend.at[mate_tok], y_s)
    fin.wait()


def solution(mesh):
    def local_step(x_loc, pos_loc, k_loc, v_loc, w_q, w_k, w_v, w_o):
        me = lax.axis_index("cp")
        p0 = pos_loc[0] - HALF * me
        row = jnp.arange(PAIR, dtype=jnp.int32)
        pos = p0 + rel_pos((me // 2) * 2 + row // TOK, row % TOK)
        inv_freq = jnp.power(F32(ROPE_BASE), -(jnp.arange(HD // 2, dtype=F32) * 2.0 / HD))
        ang = pos.astype(F32)[:, None] * inv_freq[None, :]
        vm = pltpu.VMEM
        anyspec = pl.BlockSpec(memory_space=pl.ANY)
        vspec = pl.BlockSpec(memory_space=pltpu.VMEM)
        one = ()
        dmas = ((3,), (8,), (2,), one, (8,), one, (4, 2), one, (4,), one, (4,),
                one, one, one, one, one, (4,), one, (2,), one, (8,), one, one, one, one)
        return pl.pallas_call(
            kernel,
            out_shape=jax.ShapeDtypeStruct((TOK, MODEL), BF16),
            in_specs=[anyspec, anyspec, anyspec, vspec, vspec, anyspec, anyspec, anyspec, anyspec],
            out_specs=anyspec,
            scratch_shapes=[
                vm((PAIR, MODEL), BF16),
                vm((2, CACHE, HEADS, HD), BF16),
                vm((HEADS, 2 * CACHE, HD), BF16),
                vm((4, 8, 2 * CACHE, HD), BF16),
                vm((4, 2 * CACHE, HD), BF16),
                vm((4, 8, PAIR, HD), BF16),
                vm((2, 16, HD, HD), BF16),
                vm((HEADS, HD, QB), BF16),
                vm((4, 2, HD, HD), BF16),
                vm((4, 2, PAIR, HD), BF16),
                vm((HEADS, STAT, QB), F32),
                vm((4, STAT, QB), F32),
                vm((2, STAT, QB), F32),
                vm((2, KT, QB), F32),
                vm((4, MODEL, WCOLS), BF16),
                vm((2, 4, HD, HD), BF16),
                vm((2, HEADS, HD, HD), BF16),
                vm((PAIR, QCOLS), BF16),
                vm((4, RC, HD), jnp.int32),
                vm((PAIR, OHALF), BF16),
                vm((TOK, MODEL), BF16),
            ] + [pltpu.SemaphoreType.DMA(n) for n in dmas],
            compiler_params=pltpu.CompilerParams(
                collective_id=0, has_side_effects=True, vmem_limit_bytes=67043328),
        )(x_loc, k_loc, v_loc, jnp.cos(ang), jnp.sin(ang), w_q, w_k, w_v, w_o)

    tok_spec = P(("data", "cp"), None)
    pos_spec = P(("data", "cp"))
    cache_spec = P(("data", "cp"), None, None)
    return jax.shard_map(local_step, mesh=mesh, in_specs=(tok_spec, pos_spec, cache_spec, cache_spec, P(), P(), P(), P()), out_specs=tok_spec, check_vma=False)
```
